32 devices in a mesh: row: 4 (over y, x), col: 8 (over z, core).
Axes of the slice: x: 2, y: 2, z: 4, core: 2. Of those that a mesh axis runs over, the one named last changes fastest.
Arguments:
- b_values: bfloat16 [2048, 12288], P('row', 'col'), may hold values from -0.125 to 0.125
- tile_mask: int32 [8, 48], replicated, may hold values 0 or 1
Outputs:
- factored: float32 [12288, 12288], P('row', 'col')
The draws below stay inside these ranges and needn't reach their ends.
Inputs may be any that keep to these rules, and one draw needn't show every extreme that they name: tile_mask[i, j] is 1 where tile (i, j) of B is kept and 0 where it is empty.
All inputs are finite; a program needn't handle non-finite values.
Results may differ from the reference program's by a relative error of at most 0.0017.
Values may be sent and summed in bfloat16 or wider, within the bound.
A program may use at most 128 MiB of HBM per device.

```python
import jax
import jax.numpy as jnp
from jax import lax

AUX = 12288
TILE = 256
PANEL = 512
ROWS = 2048


def place_ends(result, stream_key, least, high):
    longest = result.shape.index(max(result.shape))
    spots = []
    for shift in (0, 1):
        where = [jax.random.randint(jax.random.fold_in(stream_key, axis), (), 0, length) for axis, length in enumerate(result.shape)]
        where[longest] = (where[longest] + shift) % result.shape[longest]
        spots.append(tuple(where))
    return result.at[spots[0]].set(least).at[spots[1]].set(high)


def levels(rng, extent, shards, smallest, largest):
    def one(axis_at, parts):
        draws = jax.random.uniform(jax.random.fold_in(jax.random.fold_in(rng, 6), axis_at), (parts,), jnp.float32, smallest / len(shards), largest / len(shards))
        return jnp.repeat(jnp.exp(draws), extent[axis_at] // parts).reshape((-1,) + (1,) * (len(extent) - axis_at - 1))

    gain = one(*shards[0])
    for cut in shards[1:]:
        gain = gain * one(*cut)
    return gain


def gaussian(own_key, shape, scale, reach, pieces=(), held_as=jnp.bfloat16):
    drawn = jax.random.normal(own_key, shape, jnp.float32) * scale
    if len(pieces) > 0:
        drawn = levels(own_key, shape, pieces, -0.22, 0.18) * drawn
    return jnp.clip(drawn, min=-reach, max=reach).astype(held_as)


def setup_inputs(seed: int = 0) -> dict:
    arg_keys = jax.random.split(jax.random.key(seed), 3)
    return {
        "b_values": gaussian(arg_keys[0], (ROWS, AUX), ROWS ** -0.5, 0.125, ((0, 4), (1, 8))),
        "tile_mask": place_ends((jax.random.randint(arg_keys[1], (ROWS // TILE, AUX // TILE), 0, 4) < 3).astype(jnp.int32), jax.random.fold_in(arg_keys[1], 1), 0, 1),
    }


def expand_tiles(blocks):
    return jnp.repeat(jnp.repeat(blocks, TILE, axis=0), TILE, axis=1)

def factor_top(corner, panel):
    width = corner.shape[0]
    updated = corner
    factor = jnp.zeros_like(corner)
    for number in range(width // panel):
        lower_edge = number * panel
        upper_edge = lower_edge + panel
        diagonal_block = jnp.linalg.cholesky(updated[lower_edge:upper_edge, lower_edge:upper_edge])
        below = jax.scipy.linalg.solve_triangular(diagonal_block, updated[upper_edge:, lower_edge:upper_edge].T, lower=True).T
        factor = factor.at[lower_edge:upper_edge, lower_edge:upper_edge].set(diagonal_block)
        factor = factor.at[upper_edge:, lower_edge:upper_edge].set(below)
        updated = updated.at[upper_edge:, upper_edge:].add(-jnp.dot(below, below.T, precision=lax.Precision.HIGHEST))
    return factor

def panel_rows(source_rows, factor, panel):
    width = factor.shape[0]
    current = source_rows
    solved_parts = []
    for number in range(width // panel):
        lower_edge = number * panel
        upper_edge = lower_edge + panel
        solved = jax.scipy.linalg.solve_triangular(factor[lower_edge:upper_edge, lower_edge:upper_edge], current[:, lower_edge:upper_edge].T, lower=True).T
        solved_parts.append(solved)
        current = current.at[:, upper_edge:].add(-jnp.dot(solved, factor[upper_edge:, lower_edge:upper_edge].T, precision=lax.Precision.HIGHEST))
    return jnp.concatenate(solved_parts, axis=1)

def reference(b_values, tile_mask):
    span = 2 * PANEL
    masked = (b_values.astype(jnp.float32) * expand_tiles(tile_mask).astype(jnp.float32)).astype(jnp.bfloat16)
    product = lax.dot_general(masked.astype(jnp.float32), masked.astype(jnp.float32), (((0,), (0,)), ((), ())), preferred_element_type=jnp.float32)
    system = product + jnp.eye(AUX, dtype=jnp.float32)
    factor = factor_top(system[:span, :span], PANEL)
    lead = panel_rows(system[:, :span], factor, PANEL)
    trailing = system - jnp.dot(lead, lead.T, precision=lax.Precision.HIGHEST)
    padded = jnp.pad(lead, ((0, 0), (0, AUX - span)))
    row_ids = lax.broadcasted_iota(jnp.int32, (AUX, AUX), 0)
    col_ids = lax.broadcasted_iota(jnp.int32, (AUX, AUX), 1)
    zeros = jnp.zeros_like(system)
    return jnp.where(col_ids < span, jnp.where(row_ids >= col_ids, padded, zeros), jnp.where(row_ids < span, zeros, trailing))
```

```python
import jax
import jax.numpy as jnp
from jax import lax
from jax.experimental import pallas as pl
from jax.experimental.pallas import tpu as pltpu
from jax.sharding import PartitionSpec as P

TILE = 256
PANEL = 512
BLOCK = 128


def expand_tiles(blocks):
    return jnp.repeat(jnp.repeat(blocks, TILE, axis=0), TILE, axis=1)


def halves_of(x):
    high = lax.reduce_precision(x, 8, 7)
    return high.astype(jnp.bfloat16), (x - high).astype(jnp.bfloat16)


def product(a, b, dims):
    a_high = a.astype(jnp.bfloat16)
    b_high = b.astype(jnp.bfloat16)
    a_low = (a - a_high.astype(jnp.float32)).astype(jnp.bfloat16)
    b_low = (b - b_high.astype(jnp.float32)).astype(jnp.bfloat16)

    def one(x, y):
        return lax.dot_general(x, y, (dims, ((), ())), preferred_element_type=jnp.float32)

    return one(a_low, b_high) + one(a_high, b_low) + one(a_high, b_high)


def eliminate_group(work, group):
    first = pl.multiple_of(group * 8, 8)
    rows = work[pl.ds(first, 8), :]
    lanes = lax.broadcasted_iota(jnp.int32, (8, BLOCK), 1)
    subs = lax.broadcasted_iota(jnp.int32, (8, 1), 0)
    square = rows[:, :BLOCK]
    cols = [
        jnp.sum(jnp.where(lanes == first + t, square, 0.0), axis=1, keepdims=True)
        for t in range(8)
    ]
    scale = jnp.zeros((8, 1), jnp.float32)
    for t in range(8):
        pivot = cols[t][t : t + 1, :]
        scale = jnp.where(subs == t, lax.rsqrt(pivot), scale)
        factor = jnp.where(subs > t, cols[t] / pivot, 0.0)
        for s in range(t + 1, 8):
            cols[s] = cols[s] - factor * cols[s][t : t + 1, :]
        rows = rows - factor * rows[t : t + 1, :]
    rows = rows * scale
    high = rows.astype(jnp.bfloat16).astype(jnp.float32)
    low = rows - high
    below = lanes >= first + 8
    left_high = jnp.where(below, high[:, :BLOCK], 0.0)
    left_low = jnp.where(below, low[:, :BLOCK], 0.0)
    left = jnp.concatenate([left_low, left_low, left_high, left_high], axis=0)
    right = jnp.concatenate([low, high, low, high], axis=0)
    update = lax.dot_general(
        left.astype(jnp.bfloat16),
        right.astype(jnp.bfloat16),
        (((0,), (0,)), ((), ())),
        preferred_element_type=jnp.float32,
    )
    work[pl.ds(first, 8), :] = rows
    work[...] -= update


def factor_kernel(corner, inverse, updated, work, panel):
    span = corner.shape[0]
    updated[...] = corner[...]
    inverse[...] = jnp.zeros_like(inverse)
    row_ids = lax.broadcasted_iota(jnp.int32, (BLOCK, BLOCK), 0)
    col_ids = lax.broadcasted_iota(jnp.int32, (BLOCK, BLOCK), 1)
    for lower in range(0, span, BLOCK):
        upper = lower + BLOCK
        work[:, :BLOCK] = updated[lower:upper, lower:upper]
        work[:, BLOCK:] = jnp.where(row_ids == col_ids, 1.0, 0.0)

        @pl.loop(0, BLOCK // 8)
        def _(group):
            eliminate_group(work, group)

        own = jnp.where(row_ids >= col_ids, work[:, BLOCK:], 0.0)
        if lower > 0:
            inverse[lower:upper, :lower] = product(
                own, inverse[lower:upper, :lower], ((1,), (0,))
            )
        inverse[lower:upper, lower:upper] = own
        if upper == span:
            continue
        panel[upper:, :] = product(updated[upper:, lower:upper], own, ((1,), (1,)))

        @pl.loop(upper // BLOCK, span // BLOCK)
        def _(tile):
            at = pl.ds(pl.multiple_of(tile * BLOCK, BLOCK), BLOCK)
            part = panel[at, :]
            updated[at, upper:] -= product(part, panel[upper:, :], ((1,), (1,)))
            inverse[at, :upper] -= product(part, inverse[lower:upper, :upper], ((1,), (0,)))


def factor_inverse(corner):
    span = corner.shape[0]
    return pl.pallas_call(
        factor_kernel,
        out_shape=jax.ShapeDtypeStruct((span, span), jnp.float32),
        in_specs=[pl.BlockSpec(memory_space=pltpu.VMEM)],
        out_specs=pl.BlockSpec(memory_space=pltpu.VMEM),
        scratch_shapes=[
            pltpu.VMEM((span, span), jnp.float32),
            pltpu.VMEM((BLOCK, 2 * BLOCK), jnp.float32),
            pltpu.VMEM((span, BLOCK), jnp.float32),
        ],
        compiler_params=pltpu.CompilerParams(vmem_limit_bytes=40 * 1024 * 1024),
        cost_estimate=pl.CostEstimate(
            flops=56 * span**3, bytes_accessed=8 * span * span, transcendentals=0
        ),
    )(corner)


def on_device(nr, nc, b_values, tile_mask):
    row_index = lax.axis_index("row")
    col_index = lax.axis_index("col")
    local_rows, width = b_values.shape
    ratio = nc // nr
    height = ratio * width
    span = 2 * PANEL
    occupancy = lax.dynamic_slice(
        tile_mask,
        (row_index * (local_rows // TILE), col_index * (width // TILE)),
        (local_rows // TILE, width // TILE),
    )
    masked = b_values * expand_tiles(occupancy).astype(jnp.bfloat16)

    pieces = []
    for owner in range(-(-span // width)):
        extent = min(width, span - owner * width)
        piece = masked[:, :extent]
        piece = jnp.where(col_index == owner, piece, jnp.zeros_like(piece))
        pieces.append(lax.psum(piece, "col"))
    lead_b = lax.all_gather(jnp.concatenate(pieces, axis=1), "row", axis=0, tiled=True)

    columns = lax.all_gather(masked, "row", axis=0, tiled=True)
    perm = [
        (q * nc + ratio * r + h, r * nc + ratio * q + h)
        for q in range(nr)
        for r in range(nr)
        for h in range(ratio)
    ]
    swapped = lax.ppermute(masked, ("row", "col"), perm)
    left = lax.all_gather(swapped, "col", axis=0)
    left = left.reshape(nr, ratio, local_rows, width).transpose(0, 2, 1, 3)
    left = left.reshape(nr * local_rows, height)

    def contract(a, b):
        return lax.dot_general(
            a, b, (((0,), (0,)), ((), ())), preferred_element_type=jnp.float32
        )

    corner = contract(lead_b, lead_b) + jnp.eye(span, dtype=jnp.float32)
    inverse = factor_inverse(corner)
    strip = contract(lead_b, columns)
    solved = jnp.dot(inverse, strip, precision=lax.Precision.HIGH)
    solved = jnp.dot(inverse.T, solved, precision=lax.Precision.HIGH)
    start = jnp.minimum(col_index * width, span)
    padded = jnp.concatenate([-inverse.T, jnp.zeros((span, width), jnp.float32)], axis=1)
    own = lax.dynamic_slice_in_dim(padded, start, width, 1)
    cols = col_index * width + lax.broadcasted_iota(jnp.int32, (1, width), 1)
    weights_high, weights_low = halves_of(jnp.where(cols < span, own, solved))

    def plain(a, b):
        return jnp.dot(a, b, preferred_element_type=jnp.float32)

    right = jnp.where(cols < span, 0.0, columns.astype(jnp.float32))
    right = right - (plain(lead_b, weights_high) + plain(lead_b, weights_low))
    right_high, right_low = halves_of(right)
    total = contract(left, right_low) + contract(left, right_high)

    diagonal = jnp.concatenate([jnp.diagonal(inverse), jnp.ones((width,), jnp.float32)])
    diagonal = lax.dynamic_slice_in_dim(diagonal, start, width, 0)[None, :]
    global_rows = row_index * height + lax.broadcasted_iota(jnp.int32, (height, width), 0)
    global_cols = col_index * width + lax.broadcasted_iota(jnp.int32, (height, width), 1)
    total = total + jnp.where(global_rows == global_cols, diagonal, 0.0)
    return jnp.where(global_rows >= jnp.minimum(global_cols, span), total, 0.0)


def solution(mesh):
    nr, nc = mesh.shape["row"], mesh.shape["col"]

    def body(b_values, tile_mask):
        return on_device(nr, nc, b_values, tile_mask)

    return jax.shard_map(
        body,
        mesh=mesh,
        in_specs=(P("row", "col"), P()),
        out_specs=P("row", "col"),
        check_vma=False,
    )
```
